32 devices in a mesh: seq: 16 (over z, x, core), head: 2 (over y).
Axes of the slice: x: 2, y: 2, z: 4, core: 2. Of those that a mesh axis runs over, the one named last changes fastest.
Arguments:
- query: bfloat16 [1, 4096, 2048], P(None, 'seq', 'head'), may hold values from -210 to 210
- keys: bfloat16 [1, 4096, 512], P(None, 'seq', 'head'), may hold values from -7 to 7
- values: bfloat16 [1, 4096, 512], P(None, 'seq', 'head'), may hold values from -6 to 6
- grad_out: bfloat16 [1, 4096, 2048], P(None, 'seq', 'head'), may hold values from -6 to 6
- global_offset: int32 [1, 64], replicated, may hold values from 0 to 255, as said below
- owner: int32 [16], replicated, may hold values from 0 to 15, each once
- block_lists: int32 [1, 32, 3], P(None, 'seq'), may hold values from 0 to 31, as said below
Outputs:
- grad_query: bfloat16 [1, 4096, 2048], P(None, 'seq', 'head')
- grad_keys: bfloat16 [1, 4096, 512], P(None, 'seq', 'head')
- grad_values: bfloat16 [1, 4096, 512], P(None, 'seq', 'head')
The draws below stay inside these ranges and needn't reach their ends.
Inputs may be any that keep to these rules, and one draw needn't show every extreme that they name: `block_lists`: row b of each layer lists b first, then 3 - 1 other distinct blocks within 2 blocks of b. `global_offset`: distinct within a layer. `owner`: each sequence shard appears once.
All inputs are finite; a program needn't handle non-finite values.
Results may differ from the reference program's by a relative error of at most 0.02.
Values may be sent and summed in bfloat16 or wider, within the bound.
A program may use at most 64 MiB of HBM per device.

```python
import jax
import jax.numpy as jnp
from jax import lax

HQ = 16
HK = 4
DH = 128
LAYERS = 1
BLOCK = 128
REACH = 2
LISTED = 3
G = 64
TOK_DEV = 256
SEQ = 4096
NBLK = 32
N_SEQ = 16


def shared_draw(key):
    full_shape = (LAYERS, SEQ, HK * DH)
    base_keys = jax.random.truncated_normal(jax.random.fold_in(key, 101), -6.0, 6.0, full_shape, jnp.float32)
    return base_keys


def draw_keys(key, part):
    base_keys = shared_draw(key)
    return base_keys.astype(jnp.bfloat16)


def draw_query(key, part):
    drawn = jax.random.truncated_normal(jax.random.fold_in(key, 201), -6.0, 6.0, (LAYERS, SEQ, HQ * DH), jnp.float32)
    return drawn.astype(jnp.bfloat16)


def draw_global_offset(key, part):
    ranks = jax.random.randint(jax.random.fold_in(key, 301), (LAYERS, TOK_DEV), 0, 65536) * TOK_DEV + jnp.arange(TOK_DEV)
    unused, picked = lax.top_k(ranks, G)
    return picked.astype(jnp.int32)


def draw_block_lists(key, part):
    offsets = jnp.concatenate([jnp.arange(-REACH, 0), jnp.arange(1, REACH + 1)])
    block_ids = jnp.arange(NBLK)
    candidate = block_ids[:, None] + offsets[None, :]
    inside = (candidate >= 0) & (candidate < NBLK)
    ranks = jax.random.randint(jax.random.fold_in(key, 401), (LAYERS, NBLK, 2 * REACH), 0, 65536) * (2 * REACH) + jnp.arange(2 * REACH)
    ranks = jnp.where(inside[None], ranks, -1 - jnp.arange(2 * REACH))
    unused, picked = lax.top_k(ranks, LISTED - 1)
    others = jnp.take_along_axis(jnp.broadcast_to(candidate, (LAYERS, NBLK, 2 * REACH)), picked, axis=2)
    itself = jnp.broadcast_to(block_ids[None, :, None], (LAYERS, NBLK, 1))
    return jnp.concatenate([itself, others], axis=2).astype(jnp.int32)


def block_scale(rng, extent, pieces, low, top_value):
    loudness = 1.0
    for dim, blocks in pieces:
        steps = jax.random.uniform(jax.random.fold_in(jax.random.fold_in(rng, 6), dim), (blocks,), jnp.float32, low / len(pieces), top_value / len(pieces))
        loudness = loudness * jnp.repeat(jnp.exp(steps), extent[dim] // blocks).reshape((-1,) + (1,) * (len(extent) - 1 - dim))
    return loudness


def gaussian(stream_key, extent, spread, bound, cuts=(), dtype=jnp.bfloat16):
    drawn = spread * jax.random.normal(stream_key, extent, jnp.float32)
    if cuts:
        drawn = drawn * block_scale(stream_key, extent, cuts, -0.22, 0.18)
    return jnp.clip(drawn, -bound, bound).astype(dtype)


def setup_inputs(seed: int = 0) -> dict:
    arg_keys = jax.random.split(jax.random.key(seed), 8)
    query = draw_query(jax.random.fold_in(arg_keys[7], 71), 0)
    keys = draw_keys(jax.random.fold_in(arg_keys[7], 71), 0)
    values = gaussian(arg_keys[2], (LAYERS, SEQ, HK * DH), 1.0, 6.0, ((1, 16), (2, 2)))
    grad_out = gaussian(arg_keys[3], (LAYERS, SEQ, HQ * DH), 1.0, 6.0, ((1, 16), (2, 2)))
    global_offset = draw_global_offset(jax.random.fold_in(arg_keys[7], 71), 0)
    owner = jax.random.permutation(arg_keys[5], N_SEQ).astype(jnp.int32)
    block_lists = draw_block_lists(jax.random.fold_in(arg_keys[7], 71), 0)
    return {"query": query, "keys": keys, "values": values, "grad_out": grad_out, "global_offset": global_offset, "owner": owner, "block_lists": block_lists}


def scores(q_block, k_rows):
    return jnp.einsum("tcgd,scd->cgts", q_block.astype(jnp.float32), k_rows.astype(jnp.float32)) * (DH ** -0.5)


def backward(q_block, g_block, k_rows, v_rows, attn_probs, out_dot):
    attn_half = lax.optimization_barrier(attn_probs.astype(jnp.bfloat16))
    grad_probs = jnp.einsum("tcgd,scd->cgts", g_block.astype(jnp.float32), v_rows.astype(jnp.float32))
    grad_logits = lax.optimization_barrier((attn_probs * (grad_probs - out_dot[..., None])).astype(jnp.bfloat16))
    grad_q = jnp.einsum("cgts,scd->tcgd", grad_logits.astype(jnp.float32), k_rows.astype(jnp.float32)) * (DH ** -0.5)
    grad_k = jnp.einsum("cgts,tcgd->scd", grad_logits.astype(jnp.float32), q_block.astype(jnp.float32)) * (DH ** -0.5)
    grad_v = jnp.einsum("cgts,tcgd->scd", attn_half.astype(jnp.float32), g_block.astype(jnp.float32))
    return grad_q, grad_k, grad_v


def attend(q_block, g_block, k_rows, v_rows):
    logits = scores(q_block, k_rows)
    top_logit = jnp.max(logits, axis=-1, keepdims=True)
    log_total = top_logit + jnp.log(jnp.sum(jnp.exp(logits - top_logit), axis=-1, keepdims=True))
    attn_probs = jnp.exp(logits - log_total)
    attn_half = lax.optimization_barrier(attn_probs.astype(jnp.bfloat16))
    output = jnp.einsum("cgts,scd->tcgd", attn_half.astype(jnp.float32), v_rows.astype(jnp.float32)).astype(jnp.bfloat16)
    output = lax.optimization_barrier(output)
    out_dot = jnp.einsum("tcgd,tcgd->cgt", g_block.astype(jnp.float32), output.astype(jnp.float32))
    return backward(q_block, g_block, k_rows, v_rows, attn_probs, out_dot)


def reference(query, keys, values, grad_out, global_offset, owner, block_lists):
    group_size = HQ // HK
    window_len = LISTED * BLOCK
    kv_width = HK * DH
    grads_q = []
    grads_k = []
    grads_v = []
    for layer_idx in range(LAYERS):
        key_blocks = keys[layer_idx].reshape(NBLK, BLOCK, HK, DH)
        value_blocks = values[layer_idx].reshape(NBLK, BLOCK, HK, DH)
        global_pos = (owner[layer_idx] * TOK_DEV + global_offset[layer_idx]).astype(jnp.int32)
        global_k = keys[layer_idx][global_pos].reshape(G, HK, DH)
        global_v = values[layer_idx][global_pos].reshape(G, HK, DH)
        q_blocks = query[layer_idx].reshape(NBLK, BLOCK, HK, group_size, DH)
        g_blocks = grad_out[layer_idx].reshape(NBLK, BLOCK, HK, group_size, DH)

        def block_step(state_sums, inputs):
            sum_k, sum_v, glob_k, glob_v = state_sums
            q_block, g_block, block_idx = inputs
            block_idx = block_idx.astype(jnp.int32)
            k_rows = jnp.concatenate([key_blocks[block_idx].reshape(window_len, HK, DH), global_k], axis=0)
            v_rows = jnp.concatenate([value_blocks[block_idx].reshape(window_len, HK, DH), global_v], axis=0)
            grad_q, grad_k, grad_v = attend(q_block, g_block, k_rows, v_rows)
            sum_k = sum_k.at[block_idx].add(grad_k[:window_len].reshape(LISTED, BLOCK, kv_width))
            sum_v = sum_v.at[block_idx].add(grad_v[:window_len].reshape(LISTED, BLOCK, kv_width))
            glob_k = glob_k + grad_k[window_len:].reshape(G, kv_width)
            glob_v = glob_v + grad_v[window_len:].reshape(G, kv_width)
            return (sum_k, sum_v, glob_k, glob_v), grad_q.astype(jnp.bfloat16).reshape(BLOCK, HQ * DH)

        zero_state = (jnp.zeros((NBLK, BLOCK, kv_width), jnp.float32), jnp.zeros((NBLK, BLOCK, kv_width), jnp.float32),
                      jnp.zeros((G, kv_width), jnp.float32), jnp.zeros((G, kv_width), jnp.float32))
        final, grad_q_blocks = lax.scan(block_step, zero_state, (q_blocks, g_blocks, block_lists[layer_idx]))
        total_k = final[0].reshape(SEQ, kv_width).at[global_pos].add(final[2])
        total_v = final[1].reshape(SEQ, kv_width).at[global_pos].add(final[3])
        grads_q.append(grad_q_blocks.reshape(SEQ, HQ * DH))
        grads_k.append(total_k.astype(jnp.bfloat16))
        grads_v.append(total_v.astype(jnp.bfloat16))
    return jnp.stack(grads_q), jnp.stack(grads_k), jnp.stack(grads_v)
```

```python
import functools

import jax
import jax.numpy as jnp
from jax import lax
from jax.experimental import pallas as pl
from jax.experimental.pallas import tpu as pltpu
from jax.sharding import PartitionSpec as P

HQ = 16
HK = 4
DH = 128
BLOCK = 128
REACH = 2
PIECE = 16
LOG2E = 1.4426950408889634
F32 = jnp.float32
BF16 = jnp.bfloat16


def nt(a, b):
    return lax.dot_general(a, b, (((1,), (1,)), ((), ())), preferred_element_type=F32)


def nn(a, b):
    return lax.dot_general(a, b, (((1,), (0,)), ((), ())), preferred_element_type=F32)


def kernel(
    n, heads, group, nb, listed, gtok,
    owner_ref, lists_ref, goff_ref, q_hbm, k_hbm, v_hbm, g_hbm,
    dq_ref, dk_ref, dv_ref,
    qv, gv, gsend, hub_in, hub_out, gall, gpart, hub2_in, hub2_out, gall2,
    wslot, own, sback, rback, load_sem, big_sem, ks_sem, kr_sem, gs_sem, gr_sem, hs_sem, hr_sem,
    *kvw,
):
    me = lax.axis_index("seq")
    rpp = gtok // PIECE
    pieces = 2 * heads * rpp
    rows = nb * BLOCK
    src_refs = (k_hbm, v_hbm)

    loads = []
    for t in range(2):
        for c in range(heads):
            for i in range(nb):
                cp = pltpu.make_async_copy(
                    src_refs[t].at[0, pl.ds(i * BLOCK, BLOCK), pl.ds(c * DH, DH)],
                    kvw[t * heads + c].at[REACH + i],
                    load_sem.at[(t * heads + c) * nb + i],
                )
                cp.start()
                loads.append(cp)
    cq = pltpu.make_async_copy(q_hbm.at[0], qv, big_sem.at[0])
    cg = pltpu.make_async_copy(g_hbm.at[0], gv, big_sem.at[1])
    cq.start()
    cg.start()

    barrier = pltpu.get_barrier_semaphore()

    @pl.loop(1, n)
    def _(i):
        pl.semaphore_signal(
            barrier, inc=1, device_id={"seq": lax.rem(me + i, n)}, device_id_type=pl.DeviceIdType.MESH
        )

    for cp in loads:
        cp.wait()

    hot = lax.broadcasted_iota(jnp.int32, (rows, gtok), 0) == goff_ref[...]
    hot = jnp.where(hot, 1.0, 0.0).astype(BF16)
    for t in range(2):
        for c in range(heads):
            mine = kvw[t * heads + c][REACH : REACH + nb].reshape(rows, DH)
            got = lax.dot_general(hot, mine, (((0,), (0,)), ((), ())), preferred_element_type=F32)
            base = (t * heads + c) * rpp
            gsend[base : base + rpp] = got.astype(BF16).reshape(rpp, PIECE, DH)
    zeros_kv = jnp.zeros((REACH, BLOCK, DH), BF16)

    @pl.when(me == 0)
    def _():
        for ref in kvw:
            ref[0:REACH] = zeros_kv
        rback[0] = jnp.zeros(rback.shape[1:], BF16)

    @pl.when(me == n - 1)
    def _():
        for ref in kvw:
            ref[REACH + nb : REACH + nb + REACH] = zeros_kv
        rback[1] = jnp.zeros(rback.shape[1:], BF16)

    zero_tile = jnp.zeros((nb, 2, BLOCK, DH), F32)
    wslot[:, listed] = zero_tile

    pl.semaphore_wait(barrier, n - 1)

    def remote(src, dst, s_sem, r_sem, target):
        return pltpu.make_async_remote_copy(
            src_ref=src, dst_ref=dst, send_sem=s_sem, recv_sem=r_sem,
            device_id={"seq": target}, device_id_type=pl.DeviceIdType.MESH,
        )

    def hub_send(src, dst, s_sem, r_sem, j):
        @pl.when(j != me)
        def _():
            remote(src.at[j], dst.at[me], s_sem, r_sem, j).start()

    def drain(ref, count, sem):
        part = ref.at[pl.ds(0, count)]
        pltpu.make_async_copy(part, part, sem).wait()

    @pl.loop(0, pieces)
    def _(i):
        hub_send(gsend, hub_in, hs_sem.at[0], hr_sem.at[0], lax.rem(me + i, pieces))

    def halo(direction, c, t):
        idx = (direction * heads + c) * 2 + t
        ref = kvw[t * heads + c]
        if direction == 0:
            src, dst, target = ref.at[pl.ds(nb, REACH)], ref.at[pl.ds(0, REACH)], me + 1
        else:
            src, dst, target = ref.at[pl.ds(REACH, REACH)], ref.at[pl.ds(REACH + nb, REACH)], me - 1
        return remote(src, dst, ks_sem.at[idx], kr_sem.at[idx], target)

    def back(direction, c):
        idx = direction * heads + c
        target = me + 1 if direction == 0 else me - 1
        return remote(
            sback.at[direction, c], rback.at[direction, c], gs_sem.at[idx], gr_sem.at[idx], target
        )

    def each(direction, receiving, what):
        up = (direction == 0) != receiving
        cond = me < n - 1 if up else me > 0
        pl.when(cond)(what)

    for c in range(heads):
        for t in range(2):
            for d in range(2):
                each(d, False, lambda d=d, c=c, t=t: halo(d, c, t).start())

    @pl.when(me < pieces)
    def _():
        hub_in[me] = gsend[me]
        drain(hub_in, n - 1, hr_sem.at[0])
        pick = hub_in[owner_ref[0]]
        hub_out[...] = pick
        gall[me] = pick

        @pl.loop(1, n)
        def _(i):
            remote(hub_out, gall.at[me], hs_sem.at[1], hr_sem.at[1], lax.rem(me + i, n)).start()

        drain(gall, pieces - 1, hr_sem.at[1])

    @pl.when(me >= pieces)
    def _():
        drain(gall, pieces, hr_sem.at[1])

    cq.wait()
    cg.wait()
    scale = DH ** (-0.5)
    local_idx = [
        [
            jnp.clip(lists_ref[0, b, l] - me * nb + REACH, 0, nb + 2 * REACH - 1)
            for l in range(listed)
        ]
        for b in range(nb)
    ]
    win = listed * BLOCK
    for c in range(heads):
        for t in range(2):
            for d in range(2):
                each(d, True, lambda d=d, c=c, t=t: halo(d, c, t).wait_recv())
        kref, vref = kvw[c], kvw[heads + c]
        kg = gall[c * rpp : (c + 1) * rpp].reshape(gtok, DH)
        vg = gall[(heads + c) * rpp : (heads + c + 1) * rpp].reshape(gtok, DH)
        glob = [None, None]
        for b in range(nb):
            ks = jnp.concatenate([kref[local_idx[b][l]] for l in range(listed)] + [kg], axis=0)
            vs = jnp.concatenate([vref[local_idx[b][l]] for l in range(listed)] + [vg], axis=0)
            rsl = slice(b * BLOCK, (b + 1) * BLOCK)
            cols = [slice((c * group + i) * DH, (c * group + i + 1) * DH) for i in range(group)]
            qs = jnp.concatenate([qv[rsl, s] for s in cols], axis=0)
            gs = jnp.concatenate([gv[rsl, s] for s in cols], axis=0)
            st = nt(ks, qs)
            dp = nt(vs, gs)
            top = jnp.max(st, axis=0, keepdims=True)
            ex = jnp.exp2((st - top) * (scale * LOG2E))
            inv = 1.0 / jnp.sum(ex, axis=0, keepdims=True)
            dot = jnp.sum(ex * dp, axis=0, keepdims=True) * inv
            pr = ex * inv
            half = pr.astype(BF16)
            ds = (pr * (dp - dot)).astype(BF16)
            dv = nn(half, gs)
            dk = nn(ds, qs) * scale
            dqt = nn(ks.T, ds) * scale
            dq = dqt.T.astype(BF16)
            for i, s in enumerate(cols):
                dq_ref[0, rsl, s] = dq[i * BLOCK : (i + 1) * BLOCK]
            for t, val in enumerate((dk, dv)):
                for l in range(listed):
                    wslot[b, l, t] = val[l * BLOCK : (l + 1) * BLOCK]
                part = val[win:]
                glob[t] = part if glob[t] is None else glob[t] + part
        for t in range(2):
            base = (t * heads + c) * rpp
            gpart[base : base + rpp] = glob[t].astype(BF16).reshape(rpp, PIECE, DH)
        for dst in range(nb + 2 * REACH):
            total = None
            for b in range(nb):
                if not b <= dst <= b + 2 * REACH:
                    continue
                slot = jnp.int32(listed)
                for l in range(listed):
                    slot = jnp.where(local_idx[b][l] == dst, l, slot)
                term = wslot[b, slot]
                total = term if total is None else total + term
            if dst < REACH:
                sback[1, c, dst] = total.astype(BF16)
            elif dst < REACH + nb:
                own[c, dst - REACH] = total
            else:
                sback[0, c, dst - REACH - nb] = total.astype(BF16)
        for d in range(2):
            each(d, False, lambda d=d, c=c: back(d, c).start())
        for t in range(2):
            for r in range(rpp):
                hub_send(gpart, hub2_in, hs_sem.at[2], hr_sem.at[2], (t * heads + c) * rpp + r)

    @pl.when(me < pieces)
    def _():
        hub2_in[me] = gpart[me]
        drain(hub2_in, n - 1, hr_sem.at[2])
        total = jnp.sum(hub2_in[...].astype(F32), axis=0).astype(BF16)
        hub2_out[...] = total
        gall2[me] = total

        @pl.loop(1, n)
        def _(i):
            remote(hub2_out, gall2.at[me], hs_sem.at[3], hr_sem.at[3], lax.rem(me + i, n)).start()

        drain(gall2, pieces - 1, hr_sem.at[3])

    @pl.when(me >= pieces)
    def _():
        drain(gall2, pieces, hr_sem.at[3])

    flag = jnp.where(owner_ref[0] == me, 1.0, 0.0)
    for c in range(heads):
        for d in range(2):
            each(d, True, lambda d=d, c=c: back(d, c).wait_recv())
        for t, out in enumerate((dk_ref, dv_ref)):
            base = (t * heads + c) * rpp
            extra = nn(hot, gall2[base : base + rpp].reshape(gtok, DH)) * flag
            for i in range(nb):
                rsl = slice(i * BLOCK, (i + 1) * BLOCK)
                total = own[c, i, t] + extra[rsl]
                total = total + rback[0, c, i, t].astype(F32) + rback[1, c, i, t].astype(F32)
                out[0, rsl, c * DH : (c + 1) * DH] = total.astype(BF16)

    for c in range(heads):
        for d in range(2):
            for t in range(2):
                each(d, False, lambda d=d, c=c, t=t: halo(d, c, t).wait_send())
            each(d, False, lambda d=d, c=c: back(d, c).wait_send())

    @pl.when(me < pieces)
    def _():
        drain(gsend, pieces - 1, hs_sem.at[0])
        drain(gpart, pieces - 1, hs_sem.at[2])
        drain(hub_in, n - 1, hs_sem.at[1])
        drain(hub2_in, n - 1, hs_sem.at[3])

    @pl.when(me >= pieces)
    def _():
        drain(gsend, pieces, hs_sem.at[0])
        drain(gpart, pieces, hs_sem.at[2])


def solution(mesh):
    n = mesh.shape["seq"]

    def local(query, keys, values, grad_out, global_offset, owner, block_lists):
        rows, qw = query.shape[1:]
        kw = keys.shape[2]
        heads = kw // DH
        group = HQ // HK
        nb = rows // BLOCK
        listed = block_lists.shape[2]
        gtok = global_offset.shape[1]
        pieces = 2 * heads * gtok // PIECE
        wide = nb + 2 * REACH
        assert nb == REACH and n >= pieces
        vm = pl.BlockSpec(memory_space=pltpu.VMEM)
        sm = pl.BlockSpec(memory_space=pltpu.SMEM)
        hb = pl.BlockSpec(memory_space=pl.ANY)
        return pl.pallas_call(
            functools.partial(kernel, n, heads, group, nb, listed, gtok),
            out_shape=(
                jax.ShapeDtypeStruct(query.shape, BF16),
                jax.ShapeDtypeStruct(keys.shape, BF16),
                jax.ShapeDtypeStruct(values.shape, BF16),
            ),
            in_specs=[sm, sm, vm, hb, hb, hb, hb],
            out_specs=(vm, vm, vm),
            scratch_shapes=[
                pltpu.VMEM((rows, qw), BF16),
                pltpu.VMEM((rows, qw), BF16),
                pltpu.VMEM((pieces, PIECE, DH), BF16),
                pltpu.VMEM((n, PIECE, DH), BF16),
                pltpu.VMEM((PIECE, DH), BF16),
                pltpu.VMEM((pieces, PIECE, DH), BF16),
                pltpu.VMEM((pieces, PIECE, DH), BF16),
                pltpu.VMEM((n, PIECE, DH), BF16),
                pltpu.VMEM((PIECE, DH), BF16),
                pltpu.VMEM((pieces, PIECE, DH), BF16),
                pltpu.VMEM((nb, listed + 1, 2, BLOCK, DH), F32),
                pltpu.VMEM((heads, nb, 2, BLOCK, DH), F32),
                pltpu.VMEM((2, heads, REACH, 2, BLOCK, DH), BF16),
                pltpu.VMEM((2, heads, REACH, 2, BLOCK, DH), BF16),
                pltpu.SemaphoreType.DMA((2 * heads * nb,)),
                pltpu.SemaphoreType.DMA((2,)),
                pltpu.SemaphoreType.DMA((4 * heads,)),
                pltpu.SemaphoreType.DMA((4 * heads,)),
                pltpu.SemaphoreType.DMA((2 * heads,)),
                pltpu.SemaphoreType.DMA((2 * heads,)),
                pltpu.SemaphoreType.DMA((4,)),
                pltpu.SemaphoreType.DMA((4,)),
            ]
            + [pltpu.VMEM((wide, BLOCK, DH), BF16)] * (2 * heads),
            compiler_params=pltpu.CompilerParams(collective_id=0, has_side_effects=True),
        )(owner, block_lists, global_offset, query, keys, values, grad_out)

    return jax.shard_map(
        local,
        mesh=mesh,
        in_specs=(
            P(None, "seq", "head"),
            P(None, "seq", "head"),
            P(None, "seq", "head"),
            P(None, "seq", "head"),
            P(),
            P(),
            P(None, "seq", None),
        ),
        out_specs=(P(None, "seq", "head"), P(None, "seq", "head"), P(None, "seq", "head")),
        check_vma=False,
    )
```

```python
import functools

import jax
import jax.numpy as jnp
from jax import lax
from jax.experimental import pallas as pl
from jax.experimental.pallas import tpu as pltpu
from jax.sharding import PartitionSpec as P

HQ = 16
HK = 4
DH = 128
BLOCK = 128
REACH = 2
PIECE = 32
LOG2E = 1.4426950408889634
F32 = jnp.float32
BF16 = jnp.bfloat16


def nt(a, b):
    return lax.dot_general(a, b, (((1,), (1,)), ((), ())), preferred_element_type=F32)


def nn(a, b):
    return lax.dot_general(a, b, (((1,), (0,)), ((), ())), preferred_element_type=F32)


def kernel(
    n, heads, group, nb, listed, gtok,
    owner_ref, lists_ref, goff_ref, q_hbm, k_hbm, v_hbm, g_hbm,
    dq_ref, dk_ref, dv_ref,
    qv, gv, gsend, hub_in, hub_out, gall, gpart, hub2_in, hub2_out, gall2,
    keep_ex, keep_dp, keep_ds, wslot, own, sback, rback, load_sem, big_sem, ks_sem, kr_sem, gs_sem, gr_sem, hs_sem, hr_sem,
    *kvw,
):
    me = lax.axis_index("seq")
    rpp = gtok // PIECE
    pieces = 2 * heads * rpp
    rows = nb * BLOCK
    src_refs = (k_hbm, v_hbm)

    loads = []
    for t in range(2):
        for c in range(heads):
            for i in range(nb):
                cp = pltpu.make_async_copy(
                    src_refs[t].at[0, pl.ds(i * BLOCK, BLOCK), pl.ds(c * DH, DH)],
                    kvw[t * heads + c].at[REACH + i],
                    load_sem.at[(t * heads + c) * nb + i],
                )
                cp.start()
                loads.append(cp)
    cq = pltpu.make_async_copy(q_hbm.at[0], qv, big_sem.at[0])
    cg = pltpu.make_async_copy(g_hbm.at[0], gv, big_sem.at[1])
    cq.start()
    cg.start()

    barrier = pltpu.get_barrier_semaphore()

    first = (n - pieces) // 2
    hub = me - first

    def hubbed(i):
        return (i >= first) & (i < first + pieces)

    @pl.loop(1, n)
    def _(i):
        other = lax.rem(me + i, n)

        @pl.when(hubbed(me) | hubbed(other) | (other == me + 1) | (other == me - 1))
        def _():
            pl.semaphore_signal(
                barrier, inc=1, device_id={"seq": other}, device_id_type=pl.DeviceIdType.MESH
            )

    for cp in loads:
        cp.wait()

    hot = lax.broadcasted_iota(jnp.int32, (rows, gtok), 0) == goff_ref[...]
    hot = jnp.where(hot, 1.0, 0.0).astype(BF16)
    for t in range(2):
        for c in range(heads):
            mine = kvw[t * heads + c][REACH : REACH + nb].reshape(rows, DH)
            got = lax.dot_general(hot, mine, (((0,), (0,)), ((), ())), preferred_element_type=F32)
            base = (t * heads + c) * rpp
            gsend[base : base + rpp] = got.astype(BF16).reshape(rpp, PIECE, DH)
    zeros_kv = jnp.zeros((REACH, BLOCK, DH), BF16)

    @pl.when(me == 0)
    def _():
        for ref in kvw:
            ref[0:REACH] = zeros_kv
        rback[0] = jnp.zeros(rback.shape[1:], BF16)

    @pl.when(me == n - 1)
    def _():
        for ref in kvw:
            ref[REACH + nb : REACH + nb + REACH] = zeros_kv
        rback[1] = jnp.zeros(rback.shape[1:], BF16)

    zero_tile = jnp.zeros((nb, 2, BLOCK, DH), F32)
    wslot[:, listed] = zero_tile

    below = jnp.where((me > 0) & ~hubbed(me - 1), 1, 0)
    above = jnp.where((me < n - 1) & ~hubbed(me + 1), 1, 0)
    pl.semaphore_wait(barrier, jnp.where(hubbed(me), n - 1, pieces + below + above))

    def remote(src, dst, s_sem, r_sem, target):
        return pltpu.make_async_remote_copy(
            src_ref=src, dst_ref=dst, send_sem=s_sem, recv_sem=r_sem,
            device_id={"seq": target}, device_id_type=pl.DeviceIdType.MESH,
        )

    def hub_send(src, dst, s_sem, r_sem, j):
        @pl.when(j != hub)
        def _():
            remote(src.at[j], dst.at[me], s_sem, r_sem, first + j).start()

    def drain(ref, count, sem):
        part = ref.at[pl.ds(0, count)]
        pltpu.make_async_copy(part, part, sem).wait()

    @pl.loop(0, pieces)
    def _(i):
        hub_send(gsend, hub_in, hs_sem.at[0], hr_sem.at[0], lax.rem(me + i, pieces))

    def halo(direction, c, t):
        idx = (direction * heads + c) * 2 + t
        ref = kvw[t * heads + c]
        if direction == 0:
            src, dst, target = ref.at[pl.ds(nb, REACH)], ref.at[pl.ds(0, REACH)], me + 1
        else:
            src, dst, target = ref.at[pl.ds(REACH, REACH)], ref.at[pl.ds(REACH + nb, REACH)], me - 1
        return remote(src, dst, ks_sem.at[idx], kr_sem.at[idx], target)

    def back(direction, c):
        idx = direction * heads + c
        target = me + 1 if direction == 0 else me - 1
        return remote(
            sback.at[direction, c], rback.at[direction, c], gs_sem.at[idx], gr_sem.at[idx], target
        )

    def each(direction, receiving, what):
        up = (direction == 0) != receiving
        cond = me < n - 1 if up else me > 0
        pl.when(cond)(what)

    for c in range(heads):
        for t in range(2):
            for d in range(2):
                each(d, False, lambda d=d, c=c, t=t: halo(d, c, t).start())

    @pl.when(hubbed(me))
    def _():
        hub_in[me] = gsend[hub]
        drain(hub_in, n - 1, hr_sem.at[0])
        pick = hub_in[owner_ref[0]]
        hub_out[...] = pick
        gall[hub] = pick

        @pl.loop(1, n)
        def _(i):
            remote(hub_out, gall.at[hub], hs_sem.at[1], hr_sem.at[1], lax.rem(me + i, n)).start()

    cq.wait()
    cg.wait()
    scale = DH ** (-0.5)
    fold = scale * LOG2E
    local_idx = [
        [
            jnp.clip(lists_ref[0, b, l] - me * nb + REACH, 0, nb + 2 * REACH - 1)
            for l in range(listed)
        ]
        for b in range(nb)
    ]

    def listed_rows(t, c, b):
        return jnp.concatenate([kvw[t * heads + c][local_idx[b][l]] for l in range(listed)], axis=0)

    def global_rows(ref, t, c):
        base = (t * heads + c) * rpp
        return ref[base : base + rpp].reshape(gtok, DH)

    def columns(c):
        return [slice((c * group + i) * DH, (c * group + i + 1) * DH) for i in range(group)]

    def stacked(ref, c, b):
        rsl = slice(b * BLOCK, (b + 1) * BLOCK)
        return jnp.concatenate([ref[rsl, s] for s in columns(c)], axis=0)

    stats = {}
    for c in range(heads):
        for t in range(2):
            for d in range(2):
                each(d, True, lambda d=d, c=c, t=t: halo(d, c, t).wait_recv())
        for b in range(nb):
            st = nt(listed_rows(0, c, b), stacked(qv, c, b))
            dp = nt(listed_rows(1, c, b), stacked(gv, c, b))
            top = jnp.max(st, axis=0, keepdims=True)
            ex = jnp.exp2((st - top) * fold)
            keep_ex[c, b] = ex
            keep_dp[c, b] = dp
            stats[c, b] = (
                top,
                jnp.sum(ex, axis=0, keepdims=True),
                jnp.sum(ex * dp, axis=0, keepdims=True),
            )

    @pl.when(hubbed(me))
    def _():
        drain(gall, pieces - 1, hr_sem.at[1])

    @pl.when(~hubbed(me))
    def _():
        drain(gall, pieces, hr_sem.at[1])

    for c in range(heads):
        kg, vg = global_rows(gall, 0, c), global_rows(gall, 1, c)
        glob = [None, None]
        for b in range(nb):
            qs, gs = stacked(qv, c, b), stacked(gv, c, b)
            st = nt(kg, qs)
            dp = nt(vg, gs)
            top_w, sum_w, dot_w = stats[c, b]
            top = jnp.maximum(top_w, jnp.max(st, axis=0, keepdims=True))
            ex = jnp.exp2((st - top) * fold)
            shrink = jnp.exp2((top_w - top) * fold)
            inv = 1.0 / (sum_w * shrink + jnp.sum(ex, axis=0, keepdims=True))
            dot = (dot_w * shrink + jnp.sum(ex * dp, axis=0, keepdims=True)) * inv
            pr = ex * inv
            ds = (pr * (dp - dot)).astype(BF16)
            keep_ds[c, b] = ds
            stats[c, b] = (shrink * inv, dot)
            for t, part in enumerate((nn(ds, qs) * scale, nn(pr.astype(BF16), gs))):
                glob[t] = part if glob[t] is None else glob[t] + part
        for t in range(2):
            base = (t * heads + c) * rpp
            gpart[base : base + rpp] = glob[t].astype(BF16).reshape(rpp, PIECE, DH)

    @pl.loop(0, pieces)
    def _(i):
        hub_send(gpart, hub2_in, hs_sem.at[2], hr_sem.at[2], lax.rem(me + i, pieces))

    for c in range(heads):
        for b in range(nb):
            qs, gs = stacked(qv, c, b), stacked(gv, c, b)
            ratio, dot = stats[c, b]
            pr = keep_ex[c, b] * ratio
            ds = (pr * (keep_dp[c, b] - dot)).astype(BF16)
            dv = nn(pr.astype(BF16), gs)
            dk = nn(ds, qs) * scale
            for t, val in enumerate((dk, dv)):
                for l in range(listed):
                    wslot[b, l, t] = val[l * BLOCK : (l + 1) * BLOCK]
            ks = jnp.concatenate([listed_rows(0, c, b), global_rows(gall, 0, c)], axis=0)
            dqt = nn(ks.T, jnp.concatenate([ds, keep_ds[c, b]], axis=0)) * scale
            dq = dqt.T.astype(BF16)
            for i, s in enumerate(columns(c)):
                dq_ref[0, b * BLOCK : (b + 1) * BLOCK, s] = dq[i * BLOCK : (i + 1) * BLOCK]
        for dst in range(nb + 2 * REACH):
            total = None
            for b in range(nb):
                if not b <= dst <= b + 2 * REACH:
                    continue
                slot = jnp.int32(listed)
                for l in range(listed):
                    slot = jnp.where(local_idx[b][l] == dst, l, slot)
                term = wslot[b, slot]
                total = term if total is None else total + term
            if dst < REACH:
                sback[1, c, dst] = total.astype(BF16)
            elif dst < REACH + nb:
                own[c, dst - REACH] = total
            else:
                sback[0, c, dst - REACH - nb] = total.astype(BF16)
        for d in range(2):
            each(d, False, lambda d=d, c=c: back(d, c).start())

    @pl.when(hubbed(me))
    def _():
        hub2_in[me] = gpart[hub]
        drain(hub2_in, n - 1, hr_sem.at[2])
        total = jnp.sum(hub2_in[...].astype(F32), axis=0).astype(BF16)
        hub2_out[...] = total
        gall2[hub] = total

        @pl.loop(1, n)
        def _(i):
            remote(hub2_out, gall2.at[hub], hs_sem.at[3], hr_sem.at[3], lax.rem(me + i, n)).start()

        drain(gall2, pieces - 1, hr_sem.at[3])

    @pl.when(~hubbed(me))
    def _():
        drain(gall2, pieces, hr_sem.at[3])

    flag = jnp.where(owner_ref[0] == me, 1.0, 0.0)
    for c in range(heads):
        for d in range(2):
            each(d, True, lambda d=d, c=c: back(d, c).wait_recv())
        for t, out in enumerate((dk_ref, dv_ref)):
            extra = nn(hot, global_rows(gall2, t, c)) * flag
            for i in range(nb):
                rsl = slice(i * BLOCK, (i + 1) * BLOCK)
                total = own[c, i, t] + extra[rsl]
                total = total + rback[0, c, i, t].astype(F32) + rback[1, c, i, t].astype(F32)
                out[0, rsl, c * DH : (c + 1) * DH] = total.astype(BF16)

    for c in range(heads):
        for d in range(2):
            for t in range(2):
                each(d, False, lambda d=d, c=c, t=t: halo(d, c, t).wait_send())
            each(d, False, lambda d=d, c=c: back(d, c).wait_send())

    @pl.when(hubbed(me))
    def _():
        drain(gsend, pieces - 1, hs_sem.at[0])
        drain(gpart, pieces - 1, hs_sem.at[2])
        drain(hub_in, n - 1, hs_sem.at[1])
        drain(hub2_in, n - 1, hs_sem.at[3])

    @pl.when(~hubbed(me))
    def _():
        drain(gsend, pieces, hs_sem.at[0])
        drain(gpart, pieces, hs_sem.at[2])


def solution(mesh):
    n = mesh.shape["seq"]

    def local(query, keys, values, grad_out, global_offset, owner, block_lists):
        rows, qw = query.shape[1:]
        kw = keys.shape[2]
        heads = kw // DH
        group = HQ // HK
        nb = rows // BLOCK
        listed = block_lists.shape[2]
        gtok = global_offset.shape[1]
        pieces = 2 * heads * gtok // PIECE
        wide = nb + 2 * REACH
        assert nb == REACH and n >= pieces
        vm = pl.BlockSpec(memory_space=pltpu.VMEM)
        sm = pl.BlockSpec(memory_space=pltpu.SMEM)
        hb = pl.BlockSpec(memory_space=pl.ANY)
        return pl.pallas_call(
            functools.partial(kernel, n, heads, group, nb, listed, gtok),
            out_shape=(
                jax.ShapeDtypeStruct(query.shape, BF16),
                jax.ShapeDtypeStruct(keys.shape, BF16),
                jax.ShapeDtypeStruct(values.shape, BF16),
            ),
            in_specs=[sm, sm, vm, hb, hb, hb, hb],
            out_specs=(vm, vm, vm),
            scratch_shapes=[
                pltpu.VMEM((rows, qw), BF16),
                pltpu.VMEM((rows, qw), BF16),
                pltpu.VMEM((pieces, PIECE, DH), BF16),
                pltpu.VMEM((n, PIECE, DH), BF16),
                pltpu.VMEM((PIECE, DH), BF16),
                pltpu.VMEM((pieces, PIECE, DH), BF16),
                pltpu.VMEM((pieces, PIECE, DH), BF16),
                pltpu.VMEM((n, PIECE, DH), BF16),
                pltpu.VMEM((PIECE, DH), BF16),
                pltpu.VMEM((pieces, PIECE, DH), BF16),
                pltpu.VMEM((heads, nb, listed * BLOCK, group * BLOCK), F32),
                pltpu.VMEM((heads, nb, listed * BLOCK, group * BLOCK), F32),
                pltpu.VMEM((heads, nb, gtok, group * BLOCK), BF16),
                pltpu.VMEM((nb, listed + 1, 2, BLOCK, DH), F32),
                pltpu.VMEM((heads, nb, 2, BLOCK, DH), F32),
                pltpu.VMEM((2, heads, REACH, 2, BLOCK, DH), BF16),
                pltpu.VMEM((2, heads, REACH, 2, BLOCK, DH), BF16),
                pltpu.SemaphoreType.DMA((2 * heads * nb,)),
                pltpu.SemaphoreType.DMA((2,)),
                pltpu.SemaphoreType.DMA((4 * heads,)),
                pltpu.SemaphoreType.DMA((4 * heads,)),
                pltpu.SemaphoreType.DMA((2 * heads,)),
                pltpu.SemaphoreType.DMA((2 * heads,)),
                pltpu.SemaphoreType.DMA((4,)),
                pltpu.SemaphoreType.DMA((4,)),
            ]
            + [pltpu.VMEM((wide, BLOCK, DH), BF16)] * (2 * heads),
            compiler_params=pltpu.CompilerParams(collective_id=0, has_side_effects=True),
        )(owner, block_lists, global_offset, query, keys, values, grad_out)

    return jax.shard_map(
        local,
        mesh=mesh,
        in_specs=(
            P(None, "seq", "head"),
            P(None, "seq", "head"),
            P(None, "seq", "head"),
            P(None, "seq", "head"),
            P(),
            P(),
            P(None, "seq", None),
        ),
        out_specs=(P(None, "seq", "head"), P(None, "seq", "head"), P(None, "seq", "head")),
        check_vma=False,
    )
```

```python
import functools

import jax
import jax.numpy as jnp
from jax import lax
from jax.experimental import pallas as pl
from jax.experimental.pallas import tpu as pltpu
from jax.sharding import PartitionSpec as P

HQ = 16
HK = 4
DH = 128
BLOCK = 128
REACH = 2
PIECE = 32
LOG2E = 1.4426950408889634
F32 = jnp.float32
BF16 = jnp.bfloat16


def nt(a, b):
    return lax.dot_general(a, b, (((1,), (1,)), ((), ())), preferred_element_type=F32)


def nn(a, b):
    return lax.dot_general(a, b, (((1,), (0,)), ((), ())), preferred_element_type=F32)


def kernel(
    n, heads, group, nb, listed, gtok,
    owner_ref, lists_ref, goff_ref, q_hbm, k_hbm, v_hbm, g_hbm,
    dq_ref, dk_ref, dv_ref,
    qv, gv, gsend, hub_in, hub_out, gall, gpart, hub2_in, hub2_out, gall2,
    keep_ex, keep_dp, keep_ds, wslot, own, sback, rback, load_sem, big_sem, ks_sem, kr_sem, gs_sem, gr_sem, hs_sem, hr_sem,
    *kvw,
):
    me = lax.axis_index("seq")
    rpp = gtok // PIECE
    pieces = 2 * heads * rpp
    rows = nb * BLOCK
    src_refs = (k_hbm, v_hbm)

    loads = []
    for t in range(2):
        for c in range(heads):
            for i in range(nb):
                cp = pltpu.make_async_copy(
                    src_refs[t].at[0, pl.ds(i * BLOCK, BLOCK), pl.ds(c * DH, DH)],
                    kvw[t * heads + c].at[REACH + i],
                    load_sem.at[(t * heads + c) * nb + i],
                )
                cp.start()
                loads.append(cp)
    cq = pltpu.make_async_copy(q_hbm.at[0], qv, big_sem.at[0])
    cg = pltpu.make_async_copy(g_hbm.at[0], gv, big_sem.at[1])
    cq.start()
    cg.start()

    barrier = pltpu.get_barrier_semaphore()

    first = (n - pieces) // 2
    hub = me - first

    def hubbed(i):
        return (i >= first) & (i < first + pieces)

    @pl.loop(1, n)
    def _(i):
        other = lax.rem(me + i, n)

        @pl.when(hubbed(me) | hubbed(other) | (other == me + 1) | (other == me - 1))
        def _():
            pl.semaphore_signal(
                barrier, inc=1, device_id={"seq": other}, device_id_type=pl.DeviceIdType.MESH
            )

    for cp in loads:
        cp.wait()

    hot = lax.broadcasted_iota(jnp.int32, (rows, gtok), 0) == goff_ref[...]
    hot = jnp.where(hot, 1.0, 0.0).astype(BF16)
    for t in range(2):
        for c in range(heads):
            mine = kvw[t * heads + c][REACH : REACH + nb].reshape(rows, DH)
            got = lax.dot_general(hot, mine, (((0,), (0,)), ((), ())), preferred_element_type=F32)
            base = (t * heads + c) * rpp
            gsend[base : base + rpp] = got.astype(BF16).reshape(rpp, PIECE, DH)
    zeros_kv = jnp.zeros((REACH, BLOCK, DH), BF16)

    @pl.when(me == 0)
    def _():
        for ref in kvw:
            ref[0:REACH] = zeros_kv
        rback[0] = jnp.zeros(rback.shape[1:], BF16)

    @pl.when(me == n - 1)
    def _():
        for ref in kvw:
            ref[REACH + nb : REACH + nb + REACH] = zeros_kv
        rback[1] = jnp.zeros(rback.shape[1:], BF16)

    zero_tile = jnp.zeros((nb, 2, BLOCK, DH), F32)
    wslot[:, listed] = zero_tile

    below = jnp.where((me > 0) & ~hubbed(me - 1), 1, 0)
    above = jnp.where((me < n - 1) & ~hubbed(me + 1), 1, 0)
    pl.semaphore_wait(barrier, jnp.where(hubbed(me), n - 1, pieces + below + above))

    def remote(src, dst, s_sem, r_sem, target):
        return pltpu.make_async_remote_copy(
            src_ref=src, dst_ref=dst, send_sem=s_sem, recv_sem=r_sem,
            device_id={"seq": target}, device_id_type=pl.DeviceIdType.MESH,
        )

    def hub_send(src, dst, s_sem, r_sem, j):
        @pl.when(j != hub)
        def _():
            remote(src.at[j], dst.at[me], s_sem, r_sem, first + j).start()

    def drain(ref, count, sem):
        part = ref.at[pl.ds(0, count)]
        pltpu.make_async_copy(part, part, sem).wait()

    @pl.loop(0, pieces)
    def _(i):
        hub_send(gsend, hub_in, hs_sem.at[0], hr_sem.at[0], lax.rem(me + i, pieces))

    def halo(direction, c, t):
        idx = (direction * heads + c) * 2 + t
        ref = kvw[t * heads + c]
        if direction == 0:
            src, dst, target = ref.at[pl.ds(nb, REACH)], ref.at[pl.ds(0, REACH)], me + 1
        else:
            src, dst, target = ref.at[pl.ds(REACH, REACH)], ref.at[pl.ds(REACH + nb, REACH)], me - 1
        return remote(src, dst, ks_sem.at[idx], kr_sem.at[idx], target)

    def back(direction, c):
        idx = direction * heads + c
        target = me + 1 if direction == 0 else me - 1
        return remote(
            sback.at[direction, c], rback.at[direction, c], gs_sem.at[idx], gr_sem.at[idx], target
        )

    def each(direction, receiving, what):
        up = (direction == 0) != receiving
        cond = me < n - 1 if up else me > 0
        pl.when(cond)(what)

    for c in range(heads):
        for t in range(2):
            for d in range(2):
                each(d, False, lambda d=d, c=c, t=t: halo(d, c, t).start())

    @pl.when(hubbed(me))
    def _():
        hub_in[me] = gsend[hub]
        drain(hub_in, n - 1, hr_sem.at[0])
        pick = hub_in[owner_ref[0]]
        hub_out[...] = pick
        gall[hub] = pick

        @pl.loop(1, n)
        def _(i):
            remote(hub_out, gall.at[hub], hs_sem.at[1], hr_sem.at[1], lax.rem(me + i, n)).start()

    cq.wait()
    cg.wait()
    scale = DH ** (-0.5)
    fold = scale * LOG2E
    local_idx = [
        [
            jnp.clip(lists_ref[0, b, l] - me * nb + REACH, 0, nb + 2 * REACH - 1)
            for l in range(listed)
        ]
        for b in range(nb)
    ]

    def listed_rows(t, c, b):
        return jnp.concatenate([kvw[t * heads + c][local_idx[b][l]] for l in range(listed)], axis=0)

    def global_rows(ref, t, c):
        base = (t * heads + c) * rpp
        return ref[base : base + rpp].reshape(gtok, DH)

    def columns(c):
        return [slice((c * group + i) * DH, (c * group + i + 1) * DH) for i in range(group)]

    def stacked(ref, c, b):
        rsl = slice(b * BLOCK, (b + 1) * BLOCK)
        return jnp.concatenate([ref[rsl, s] for s in columns(c)], axis=0)

    stats = {}
    for c in range(heads):
        for t in range(2):
            for d in range(2):
                each(d, True, lambda d=d, c=c, t=t: halo(d, c, t).wait_recv())
        for b in range(nb):
            st = nt(listed_rows(0, c, b), stacked(qv, c, b))
            dp = nt(listed_rows(1, c, b), stacked(gv, c, b))
            top = jnp.max(st, axis=0, keepdims=True)
            ex = jnp.exp2((st - top) * fold)
            keep_ex[c, b] = ex
            keep_dp[c, b] = dp
            stats[c, b] = (
                top,
                jnp.sum(ex, axis=0, keepdims=True),
                jnp.sum(ex * dp, axis=0, keepdims=True),
            )

    @pl.when(hubbed(me))
    def _():
        drain(gall, pieces - 1, hr_sem.at[1])

    @pl.when(~hubbed(me))
    def _():
        drain(gall, pieces, hr_sem.at[1])

    for c in range(heads):
        kg, vg = global_rows(gall, 0, c), global_rows(gall, 1, c)
        glob = [None, None]
        for b in range(nb):
            qs, gs = stacked(qv, c, b), stacked(gv, c, b)
            st = nt(kg, qs)
            dp = nt(vg, gs)
            top_w, sum_w, dot_w = stats[c, b]
            top = jnp.maximum(top_w, jnp.max(st, axis=0, keepdims=True))
            ex = jnp.exp2((st - top) * fold)
            shrink = jnp.exp2((top_w - top) * fold)
            inv = 1.0 / (sum_w * shrink + jnp.sum(ex, axis=0, keepdims=True))
            dot = (dot_w * shrink + jnp.sum(ex * dp, axis=0, keepdims=True)) * inv
            pr = ex * inv
            ds = (pr * (dp - dot)).astype(BF16)
            keep_ds[c, b] = ds
            stats[c, b] = (shrink * inv, dot)
            for t, part in enumerate((nn(ds, qs) * scale, nn(pr.astype(BF16), gs))):
                glob[t] = part if glob[t] is None else glob[t] + part
        for t in range(2):
            base = (t * heads + c) * rpp
            gpart[base : base + rpp] = glob[t].astype(BF16).reshape(rpp, PIECE, DH)

    @pl.loop(0, pieces)
    def _(i):
        hub_send(gpart, hub2_in, hs_sem.at[2], hr_sem.at[2], lax.rem(me + i, pieces))

    for c in range(heads):
        for b in range(nb):
            qs, gs = stacked(qv, c, b), stacked(gv, c, b)
            ratio, dot = stats[c, b]
            pr = keep_ex[c, b] * ratio
            ds = (pr * (keep_dp[c, b] - dot)).astype(BF16)
            dv = nn(pr.astype(BF16), gs)
            dk = nn(ds, qs) * scale
            for t, val in enumerate((dk, dv)):
                for l in range(listed):
                    wslot[b, l, t] = val[l * BLOCK : (l + 1) * BLOCK]
            ks = jnp.concatenate([listed_rows(0, c, b), global_rows(gall, 0, c)], axis=0)
            dqt = nn(ks.T, jnp.concatenate([ds, keep_ds[c, b]], axis=0)) * scale
            dq = dqt.T.astype(BF16)
            for i, s in enumerate(columns(c)):
                dq_ref[0, b * BLOCK : (b + 1) * BLOCK, s] = dq[i * BLOCK : (i + 1) * BLOCK]
        for dst in range(nb + 2 * REACH):
            total = None
            for b in range(nb):
                if not b <= dst <= b + 2 * REACH:
                    continue
                slot = jnp.int32(listed)
                for l in range(listed):
                    slot = jnp.where(local_idx[b][l] == dst, l, slot)
                term = wslot[b, slot]
                total = term if total is None else total + term
            if dst < REACH:
                sback[1, c, dst] = total.astype(BF16)
            elif dst < REACH + nb:
                own[c, dst - REACH] = total
            else:
                sback[0, c, dst - REACH - nb] = total.astype(BF16)
        for d in range(2):
            each(d, False, lambda d=d, c=c: back(d, c).start())

    @pl.when(hubbed(me))
    def _():
        hub2_in[me] = gpart[hub]
        drain(hub2_in, n - 1, hr_sem.at[2])
        total = jnp.sum(hub2_in[...].astype(F32), axis=0).astype(BF16)
        hub2_out[...] = total
        gall2[hub] = total

        @pl.loop(1, n)
        def _(i):
            remote(hub2_out, gall2.at[hub], hs_sem.at[3], hr_sem.at[3], lax.rem(me + i, n)).start()

        drain(gall2, pieces - 1, hr_sem.at[3])

    @pl.when(~hubbed(me))
    def _():
        drain(gall2, pieces, hr_sem.at[3])

    flag = jnp.where(owner_ref[0] == me, 1.0, 0.0)
    for c in range(heads):
        for d in range(2):
            each(d, True, lambda d=d, c=c: back(d, c).wait_recv())
        for t, out in enumerate((dk_ref, dv_ref)):
            extra = nn(hot, global_rows(gall2, t, c)) * flag
            for i in range(nb):
                rsl = slice(i * BLOCK, (i + 1) * BLOCK)
                total = own[c, i, t] + extra[rsl]
                total = total + rback[0, c, i, t].astype(F32) + rback[1, c, i, t].astype(F32)
                out[0, rsl, c * DH : (c + 1) * DH] = total.astype(BF16)

    for c in range(heads):
        for d in range(2):
            for t in range(2):
                each(d, False, lambda d=d, c=c, t=t: halo(d, c, t).wait_send())
            each(d, False, lambda d=d, c=c: back(d, c).wait_send())

    @pl.when(hubbed(me))
    def _():
        drain(gsend, pieces - 1, hs_sem.at[0])
        drain(gpart, pieces - 1, hs_sem.at[2])
        drain(hub_in, n - 1, hs_sem.at[1])
        drain(hub2_in, n - 1, hs_sem.at[3])

    @pl.when(~hubbed(me))
    def _():
        drain(gsend, pieces, hs_sem.at[0])
        drain(gpart, pieces, hs_sem.at[2])


def write_out(*refs):
    copies = [
        pltpu.make_async_copy(refs[i], refs[3 + i], refs[6].at[i]) for i in range(3)
    ]
    for cp in copies:
        cp.start()
    for cp in copies:
        cp.wait()


def solution(mesh):
    n = mesh.shape["seq"]

    def local(query, keys, values, grad_out, global_offset, owner, block_lists):
        rows, qw = query.shape[1:]
        kw = keys.shape[2]
        heads = kw // DH
        group = HQ // HK
        nb = rows // BLOCK
        listed = block_lists.shape[2]
        gtok = global_offset.shape[1]
        pieces = 2 * heads * gtok // PIECE
        wide = nb + 2 * REACH
        assert nb == REACH and n >= pieces
        vm = pl.BlockSpec(memory_space=pltpu.VMEM)
        sm = pl.BlockSpec(memory_space=pltpu.SMEM)
        hb = pl.BlockSpec(memory_space=pl.ANY)
        held = pl.pallas_call(
            functools.partial(kernel, n, heads, group, nb, listed, gtok),
            out_shape=tuple(pltpu.VMEM(a.shape, BF16) for a in (query, keys, values)),
            in_specs=[sm, sm, vm, hb, hb, hb, hb],
            out_specs=(vm, vm, vm),
            scratch_shapes=[
                pltpu.VMEM((rows, qw), BF16),
                pltpu.VMEM((rows, qw), BF16),
                pltpu.VMEM((pieces, PIECE, DH), BF16),
                pltpu.VMEM((n, PIECE, DH), BF16),
                pltpu.VMEM((PIECE, DH), BF16),
                pltpu.VMEM((pieces, PIECE, DH), BF16),
                pltpu.VMEM((pieces, PIECE, DH), BF16),
                pltpu.VMEM((n, PIECE, DH), BF16),
                pltpu.VMEM((PIECE, DH), BF16),
                pltpu.VMEM((pieces, PIECE, DH), BF16),
                pltpu.VMEM((heads, nb, listed * BLOCK, group * BLOCK), F32),
                pltpu.VMEM((heads, nb, listed * BLOCK, group * BLOCK), F32),
                pltpu.VMEM((heads, nb, gtok, group * BLOCK), BF16),
                pltpu.VMEM((nb, listed + 1, 2, BLOCK, DH), F32),
                pltpu.VMEM((heads, nb, 2, BLOCK, DH), F32),
                pltpu.VMEM((2, heads, REACH, 2, BLOCK, DH), BF16),
                pltpu.VMEM((2, heads, REACH, 2, BLOCK, DH), BF16),
                pltpu.SemaphoreType.DMA((2 * heads * nb,)),
                pltpu.SemaphoreType.DMA((2,)),
                pltpu.SemaphoreType.DMA((4 * heads,)),
                pltpu.SemaphoreType.DMA((4 * heads,)),
                pltpu.SemaphoreType.DMA((2 * heads,)),
                pltpu.SemaphoreType.DMA((2 * heads,)),
                pltpu.SemaphoreType.DMA((4,)),
                pltpu.SemaphoreType.DMA((4,)),
            ]
            + [pltpu.VMEM((wide, BLOCK, DH), BF16)] * (2 * heads),
            compiler_params=pltpu.CompilerParams(collective_id=0, has_side_effects=True),
        )(owner, block_lists, global_offset, query, keys, values, grad_out)
        return pl.pallas_call(
            write_out,
            out_shape=tuple(jax.ShapeDtypeStruct(a.shape, BF16) for a in (query, keys, values)),
            in_specs=[hb] * 3,
            out_specs=[hb] * 3,
            scratch_shapes=[pltpu.SemaphoreType.DMA((3,))],
        )(*[pltpu.with_memory_space_constraint(a, pltpu.VMEM) for a in held])

    return jax.shard_map(
        local,
        mesh=mesh,
        in_specs=(
            P(None, "seq", "head"),
            P(None, "seq", "head"),
            P(None, "seq", "head"),
            P(None, "seq", "head"),
            P(),
            P(),
            P(None, "seq", None),
        ),
        out_specs=(P(None, "seq", "head"), P(None, "seq", "head"), P(None, "seq", "head")),
        check_vma=False,
    )
```

```python
import functools

import jax
import jax.numpy as jnp
from jax import lax
from jax.experimental import pallas as pl
from jax.experimental.pallas import tpu as pltpu
from jax.sharding import PartitionSpec as P

HQ = 16
HK = 4
DH = 128
BLOCK = 128
REACH = 2
PIECE = 32
LOG2E = 1.4426950408889634
F32 = jnp.float32
BF16 = jnp.bfloat16


def nt(a, b):
    return lax.dot_general(a, b, (((1,), (1,)), ((), ())), preferred_element_type=F32)


def nn(a, b):
    return lax.dot_general(a, b, (((1,), (0,)), ((), ())), preferred_element_type=F32)


def kernel(
    n, heads, group, nb, listed, gtok,
    owner_ref, lists_ref, goff_ref, q_hbm, k_hbm, v_hbm, g_hbm,
    dq_ref, dk_ref, dv_ref,
    qv, gv, gsend, hub_in, hub_out, gall, gpart, hub2_in, hub2_out, gall2,
    keep_ex, keep_dp, keep_ds, wslot, own, sback, rback, load_sem, big_sem, ks_sem, kr_sem, gs_sem, gr_sem, hs_sem, hr_sem,
    *kvw,
):
    me = lax.axis_index("seq")
    rpp = gtok // PIECE
    pieces = 2 * heads * rpp
    rows = nb * BLOCK
    src_refs = (k_hbm, v_hbm)

    loads = []
    for t in range(2):
        for c in range(heads):
            for i in range(nb):
                cp = pltpu.make_async_copy(
                    src_refs[t].at[0, pl.ds(i * BLOCK, BLOCK), pl.ds(c * DH, DH)],
                    kvw[t * heads + c].at[REACH + i],
                    load_sem.at[(t * heads + c) * nb + i],
                )
                cp.start()
                loads.append(cp)
    cq = pltpu.make_async_copy(q_hbm.at[0], qv, big_sem.at[0])
    cg = pltpu.make_async_copy(g_hbm.at[0], gv, big_sem.at[1])
    cq.start()
    cg.start()

    barrier = pltpu.get_barrier_semaphore()

    first = (n - pieces) // 2
    hub = me - first

    def hubbed(i):
        return (i >= first) & (i < first + pieces)

    @pl.loop(1, n)
    def _(i):
        other = lax.rem(me + i, n)

        @pl.when(hubbed(me) | hubbed(other) | (other == me + 1) | (other == me - 1))
        def _():
            pl.semaphore_signal(
                barrier, inc=1, device_id={"seq": other}, device_id_type=pl.DeviceIdType.MESH
            )

    for cp in loads:
        cp.wait()

    hot = lax.broadcasted_iota(jnp.int32, (rows, gtok), 0) == goff_ref[...]
    hot = jnp.where(hot, 1.0, 0.0).astype(BF16)
    for t in range(2):
        for c in range(heads):
            mine = kvw[t * heads + c][REACH : REACH + nb].reshape(rows, DH)
            got = lax.dot_general(hot, mine, (((0,), (0,)), ((), ())), preferred_element_type=F32)
            base = (t * heads + c) * rpp
            gsend[base : base + rpp] = got.astype(BF16).reshape(rpp, PIECE, DH)
    zeros_kv = jnp.zeros((REACH, BLOCK, DH), BF16)

    @pl.when(me == 0)
    def _():
        for ref in kvw:
            ref[0:REACH] = zeros_kv
        rback[0] = jnp.zeros(rback.shape[1:], BF16)

    @pl.when(me == n - 1)
    def _():
        for ref in kvw:
            ref[REACH + nb : REACH + nb + REACH] = zeros_kv
        rback[1] = jnp.zeros(rback.shape[1:], BF16)

    zero_tile = jnp.zeros((nb, 2, BLOCK, DH), F32)
    wslot[:, listed] = zero_tile

    below = jnp.where((me > 0) & ~hubbed(me - 1), 1, 0)
    above = jnp.where((me < n - 1) & ~hubbed(me + 1), 1, 0)
    pl.semaphore_wait(barrier, jnp.where(hubbed(me), n - 1, pieces + below + above))

    def remote(src, dst, s_sem, r_sem, target):
        return pltpu.make_async_remote_copy(
            src_ref=src, dst_ref=dst, send_sem=s_sem, recv_sem=r_sem,
            device_id={"seq": target}, device_id_type=pl.DeviceIdType.MESH,
        )

    def hub_send(src, dst, s_sem, r_sem, j):
        @pl.when(j != hub)
        def _():
            remote(src.at[j], dst.at[me], s_sem, r_sem, first + j).start()

    def drain(ref, count, sem):
        part = ref.at[pl.ds(0, count)]
        pltpu.make_async_copy(part, part, sem).wait()

    @pl.loop(0, pieces)
    def _(i):
        hub_send(gsend, hub_in, hs_sem.at[0], hr_sem.at[0], lax.rem(me + i, pieces))

    def halo(direction, c, t):
        idx = (direction * heads + c) * 2 + t
        ref = kvw[t * heads + c]
        if direction == 0:
            src, dst, target = ref.at[pl.ds(nb, REACH)], ref.at[pl.ds(0, REACH)], me + 1
        else:
            src, dst, target = ref.at[pl.ds(REACH, REACH)], ref.at[pl.ds(REACH + nb, REACH)], me - 1
        return remote(src, dst, ks_sem.at[idx], kr_sem.at[idx], target)

    def back(direction, c):
        idx = direction * heads + c
        target = me + 1 if direction == 0 else me - 1
        return remote(
            sback.at[direction, c], rback.at[direction, c], gs_sem.at[idx], gr_sem.at[idx], target
        )

    def each(direction, receiving, what):
        up = (direction == 0) != receiving
        cond = me < n - 1 if up else me > 0
        pl.when(cond)(what)

    for c in range(heads):
        for t in range(2):
            for d in range(2):
                each(d, False, lambda d=d, c=c, t=t: halo(d, c, t).start())

    @pl.when(hubbed(me))
    def _():
        hub_in[me] = gsend[hub]
        drain(hub_in, n - 1, hr_sem.at[0])
        pick = hub_in[owner_ref[0]]
        hub_out[...] = pick
        gall[hub] = pick

        @pl.loop(1, n)
        def _(i):
            remote(hub_out, gall.at[hub], hs_sem.at[1], hr_sem.at[1], lax.rem(me + i, n)).start()

    cq.wait()
    cg.wait()
    scale = DH ** (-0.5)
    fold = scale * LOG2E
    local_idx = [
        [
            jnp.clip(lists_ref[0, b, l] - me * nb + REACH, 0, nb + 2 * REACH - 1)
            for l in range(listed)
        ]
        for b in range(nb)
    ]

    def listed_rows(t, c, b):
        return jnp.concatenate([kvw[t * heads + c][local_idx[b][l]] for l in range(listed)], axis=0)

    def global_rows(ref, t, c):
        base = (t * heads + c) * rpp
        return ref[base : base + rpp].reshape(gtok, DH)

    def columns(c):
        return [slice((c * group + i) * DH, (c * group + i + 1) * DH) for i in range(group)]

    def stacked(ref, c, b):
        rsl = slice(b * BLOCK, (b + 1) * BLOCK)
        return jnp.concatenate([ref[rsl, s] for s in columns(c)], axis=0)

    stats = {}
    for c in range(heads):
        for d in range(2):
            each(d, True, lambda d=d, c=c: halo(d, c, 0).wait_recv())
        for b in range(nb):
            st = nt(listed_rows(0, c, b), stacked(qv, c, b))
            top = jnp.max(st, axis=0, keepdims=True)
            ex = jnp.exp2((st - top) * fold)
            keep_ex[c, b] = ex
            stats[c, b] = (top, jnp.sum(ex, axis=0, keepdims=True))
        for d in range(2):
            each(d, True, lambda d=d, c=c: halo(d, c, 1).wait_recv())
        for b in range(nb):
            dp = nt(listed_rows(1, c, b), stacked(gv, c, b))
            keep_dp[c, b] = dp
            stats[c, b] += (jnp.sum(keep_ex[c, b] * dp, axis=0, keepdims=True),)

    @pl.when(hubbed(me))
    def _():
        drain(gall, pieces - 1, hr_sem.at[1])

    @pl.when(~hubbed(me))
    def _():
        drain(gall, pieces, hr_sem.at[1])

    for c in range(heads):
        kg, vg = global_rows(gall, 0, c), global_rows(gall, 1, c)
        glob = [None, None]
        for b in range(nb):
            qs, gs = stacked(qv, c, b), stacked(gv, c, b)
            st = nt(kg, qs)
            dp = nt(vg, gs)
            top_w, sum_w, dot_w = stats[c, b]
            top = jnp.maximum(top_w, jnp.max(st, axis=0, keepdims=True))
            ex = jnp.exp2((st - top) * fold)
            shrink = jnp.exp2((top_w - top) * fold)
            inv = 1.0 / (sum_w * shrink + jnp.sum(ex, axis=0, keepdims=True))
            dot = (dot_w * shrink + jnp.sum(ex * dp, axis=0, keepdims=True)) * inv
            pr = ex * inv
            ds = (pr * (dp - dot)).astype(BF16)
            keep_ds[c, b] = ds
            stats[c, b] = (shrink * inv, dot)
            for t, part in enumerate((nn(ds, qs) * scale, nn(pr.astype(BF16), gs))):
                glob[t] = part if glob[t] is None else glob[t] + part
        for t in range(2):
            base = (t * heads + c) * rpp
            gpart[base : base + rpp] = glob[t].astype(BF16).reshape(rpp, PIECE, DH)

    @pl.loop(0, pieces)
    def _(i):
        hub_send(gpart, hub2_in, hs_sem.at[2], hr_sem.at[2], lax.rem(me + i, pieces))

    for c in range(heads):
        for b in range(nb):
            qs, gs = stacked(qv, c, b), stacked(gv, c, b)
            ratio, dot = stats[c, b]
            pr = keep_ex[c, b] * ratio
            ds = (pr * (keep_dp[c, b] - dot)).astype(BF16)
            dv = nn(pr.astype(BF16), gs)
            dk = nn(ds, qs) * scale
            for t, val in enumerate((dk, dv)):
                for l in range(listed):
                    wslot[b, l, t] = val[l * BLOCK : (l + 1) * BLOCK]
            ks = jnp.concatenate([listed_rows(0, c, b), global_rows(gall, 0, c)], axis=0)
            dqt = nn(ks.T, jnp.concatenate([ds, keep_ds[c, b]], axis=0)) * scale
            dq = dqt.T.astype(BF16)
            for i, s in enumerate(columns(c)):
                dq_ref[0, b * BLOCK : (b + 1) * BLOCK, s] = dq[i * BLOCK : (i + 1) * BLOCK]
        for dst in range(nb + 2 * REACH):
            total = None
            for b in range(nb):
                if not b <= dst <= b + 2 * REACH:
                    continue
                slot = jnp.int32(listed)
                for l in range(listed):
                    slot = jnp.where(local_idx[b][l] == dst, l, slot)
                term = wslot[b, slot]
                total = term if total is None else total + term
            if dst < REACH:
                sback[1, c, dst] = total.astype(BF16)
            elif dst < REACH + nb:
                own[c, dst - REACH] = total
            else:
                sback[0, c, dst - REACH - nb] = total.astype(BF16)
        for d in range(2):
            each(d, False, lambda d=d, c=c: back(d, c).start())

    @pl.when(hubbed(me))
    def _():
        hub2_in[me] = gpart[hub]
        drain(hub2_in, n - 1, hr_sem.at[2])
        total = jnp.sum(hub2_in[...].astype(F32), axis=0).astype(BF16)
        hub2_out[...] = total
        gall2[hub] = total

        @pl.loop(1, n)
        def _(i):
            remote(hub2_out, gall2.at[hub], hs_sem.at[3], hr_sem.at[3], lax.rem(me + i, n)).start()

        drain(gall2, pieces - 1, hr_sem.at[3])

    @pl.when(~hubbed(me))
    def _():
        drain(gall2, pieces, hr_sem.at[3])

    flag = jnp.where(owner_ref[0] == me, 1.0, 0.0)
    for c in range(heads):
        for d in range(2):
            each(d, True, lambda d=d, c=c: back(d, c).wait_recv())
        for t, out in enumerate((dk_ref, dv_ref)):
            extra = nn(hot, global_rows(gall2, t, c)) * flag
            for i in range(nb):
                rsl = slice(i * BLOCK, (i + 1) * BLOCK)
                total = own[c, i, t] + extra[rsl]
                total = total + rback[0, c, i, t].astype(F32) + rback[1, c, i, t].astype(F32)
                out[0, rsl, c * DH : (c + 1) * DH] = total.astype(BF16)

    for c in range(heads):
        for d in range(2):
            for t in range(2):
                each(d, False, lambda d=d, c=c, t=t: halo(d, c, t).wait_send())
            each(d, False, lambda d=d, c=c: back(d, c).wait_send())

    @pl.when(hubbed(me))
    def _():
        drain(gsend, pieces - 1, hs_sem.at[0])
        drain(gpart, pieces - 1, hs_sem.at[2])
        drain(hub_in, n - 1, hs_sem.at[1])
        drain(hub2_in, n - 1, hs_sem.at[3])

    @pl.when(~hubbed(me))
    def _():
        drain(gsend, pieces, hs_sem.at[0])
        drain(gpart, pieces, hs_sem.at[2])


def write_out(*refs):
    copies = [
        pltpu.make_async_copy(refs[i], refs[3 + i], refs[6].at[i]) for i in range(3)
    ]
    for cp in copies:
        cp.start()
    for cp in copies:
        cp.wait()


def solution(mesh):
    n = mesh.shape["seq"]

    def local(query, keys, values, grad_out, global_offset, owner, block_lists):
        rows, qw = query.shape[1:]
        kw = keys.shape[2]
        heads = kw // DH
        group = HQ // HK
        nb = rows // BLOCK
        listed = block_lists.shape[2]
        gtok = global_offset.shape[1]
        pieces = 2 * heads * gtok // PIECE
        wide = nb + 2 * REACH
        assert nb == REACH and n >= pieces
        vm = pl.BlockSpec(memory_space=pltpu.VMEM)
        sm = pl.BlockSpec(memory_space=pltpu.SMEM)
        hb = pl.BlockSpec(memory_space=pl.ANY)
        held = pl.pallas_call(
            functools.partial(kernel, n, heads, group, nb, listed, gtok),
            out_shape=tuple(pltpu.VMEM(a.shape, BF16) for a in (query, keys, values)),
            in_specs=[sm, sm, vm, hb, hb, hb, hb],
            out_specs=(vm, vm, vm),
            scratch_shapes=[
                pltpu.VMEM((rows, qw), BF16),
                pltpu.VMEM((rows, qw), BF16),
                pltpu.VMEM((pieces, PIECE, DH), BF16),
                pltpu.VMEM((n, PIECE, DH), BF16),
                pltpu.VMEM((PIECE, DH), BF16),
                pltpu.VMEM((pieces, PIECE, DH), BF16),
                pltpu.VMEM((pieces, PIECE, DH), BF16),
                pltpu.VMEM((n, PIECE, DH), BF16),
                pltpu.VMEM((PIECE, DH), BF16),
                pltpu.VMEM((pieces, PIECE, DH), BF16),
                pltpu.VMEM((heads, nb, listed * BLOCK, group * BLOCK), F32),
                pltpu.VMEM((heads, nb, listed * BLOCK, group * BLOCK), F32),
                pltpu.VMEM((heads, nb, gtok, group * BLOCK), BF16),
                pltpu.VMEM((nb, listed + 1, 2, BLOCK, DH), F32),
                pltpu.VMEM((heads, nb, 2, BLOCK, DH), F32),
                pltpu.VMEM((2, heads, REACH, 2, BLOCK, DH), BF16),
                pltpu.VMEM((2, heads, REACH, 2, BLOCK, DH), BF16),
                pltpu.SemaphoreType.DMA((2 * heads * nb,)),
                pltpu.SemaphoreType.DMA((2,)),
                pltpu.SemaphoreType.DMA((4 * heads,)),
                pltpu.SemaphoreType.DMA((4 * heads,)),
                pltpu.SemaphoreType.DMA((2 * heads,)),
                pltpu.SemaphoreType.DMA((2 * heads,)),
                pltpu.SemaphoreType.DMA((4,)),
                pltpu.SemaphoreType.DMA((4,)),
            ]
            + [pltpu.VMEM((wide, BLOCK, DH), BF16)] * (2 * heads),
            compiler_params=pltpu.CompilerParams(collective_id=0, has_side_effects=True),
        )(owner, block_lists, global_offset, query, keys, values, grad_out)
        return pl.pallas_call(
            write_out,
            out_shape=tuple(jax.ShapeDtypeStruct(a.shape, BF16) for a in (query, keys, values)),
            in_specs=[hb] * 3,
            out_specs=[hb] * 3,
            scratch_shapes=[pltpu.SemaphoreType.DMA((3,))],
        )(*[pltpu.with_memory_space_constraint(a, pltpu.VMEM) for a in held])

    return jax.shard_map(
        local,
        mesh=mesh,
        in_specs=(
            P(None, "seq", "head"),
            P(None, "seq", "head"),
            P(None, "seq", "head"),
            P(None, "seq", "head"),
            P(),
            P(),
            P(None, "seq", None),
        ),
        out_specs=(P(None, "seq", "head"), P(None, "seq", "head"), P(None, "seq", "head")),
        check_vma=False,
    )
```
